1024 devices in a mesh: ab: 32 (over z_lo, x, core), kl: 4 (over z_hi), ij: 8 (over y).
Axes of the slice: x: 8, y: 8, z: 8 (z_hi: 4, z_lo: 2; z = z_hi * 2 + z_lo), core: 2. Of those that a mesh axis runs over, the one named last changes fastest.
Arguments:
- amplitudes: bfloat16 [16384, 8192], P('ab', ('kl', 'ij')), may hold values from -6 to 6
- integrals: bfloat16 [8192, 8192], P(('kl', 'ab'), 'ij'), may hold values from -0.0625 to 0.0625
Outputs:
- ladder: float32 [16384, 8192], P('ab', ('ij', 'kl'))
The draws below stay inside these ranges and needn't reach their ends.
All inputs are finite; a program needn't handle non-finite values.
Results may differ from the reference program's by a relative error of at most 0.0003.
Values may be sent and summed in bfloat16 or wider, within the bound.
No kernel may reach another device: no remote copies, remote signals or barrier semaphores. Data moves between devices by JAX's collectives and lax.ppermute only.
A program may use at most 32 MiB of HBM per device.

```python
import jax
import jax.numpy as jnp
from jax import lax

PAIRS = 8128
PADDED = 8192
VPAIRS = 16384


def block_scale(stream_key, extent, cuts, smallest, high):
    gain = 1.0
    for dim, shards_of in cuts:
        heights = jax.random.uniform(jax.random.fold_in(jax.random.fold_in(stream_key, 6), dim), (shards_of,), jnp.float32, smallest / len(cuts), high / len(cuts))
        gain = gain * jnp.repeat(jnp.exp(heights), extent[dim] // shards_of).reshape((-1,) + (1,) * (len(extent) - 1 - dim))
    return gain


def noise(rng, extent, spread, most, pieces=(), held_as=jnp.bfloat16):
    entries = jax.random.normal(rng, extent, jnp.float32) * spread
    if len(pieces) > 0:
        entries = block_scale(rng, extent, pieces, -0.22, 0.18) * entries
    return jnp.clip(entries, min=-most, max=most).astype(held_as)


def setup_inputs(seed: int = 0) -> dict:
    arg_keys = jax.random.split(jax.random.key(seed), 3)
    amplitudes = noise(arg_keys[0], (VPAIRS, PADDED), 1.0, 6.0, ((0, 32), (1, 32)))
    integrals = noise(arg_keys[1], (PADDED, PADDED), PAIRS ** -0.5, 0.0625, ((0, 128), (1, 8)))
    return {"amplitudes": amplitudes, "integrals": integrals}


def reference(amplitudes, integrals):
    keep = jnp.arange(PADDED) < PAIRS
    left = jnp.where(keep[None, :], amplitudes.astype(jnp.float32), jnp.float32(0.0))
    full = jnp.dot(left, integrals.astype(jnp.float32), precision=lax.Precision.HIGHEST)
    return jnp.where(keep[None, :], full, jnp.float32(0.0))
```

```python
import jax
import jax.numpy as jnp
from jax import lax
from jax.experimental import pallas as pl
from jax.experimental.pallas import tpu as pltpu
from jax.sharding import Mesh
from jax.sharding import PartitionSpec as P

PAIRS = 8128
AXES = ("zl", "x", "c", "kl", "ij")
SCALE = 64.0
HALVES = 2

Y_PARITY = [list(range(p, 8, 2)) for p in range(2)]
X_PARITY = [[zl * 8 + x for zl in range(2) for x in range(p, 8, 2)] for p in range(2)]
Y_HOP = [(c * 8 + y, c * 8 + (y + 1 - 2 * c) % 8) for c in range(2) for y in range(8)]
X_HOP = [(x * 2 + c, (x + 1 - 2 * c) % 8 * 2 + c) for c in range(2) for x in range(8)]
SWAP = [(0, 1), (1, 0)]


def to_all(shard, axes, groups, size):
    return lax.all_to_all(
        jnp.broadcast_to(shard[None], (size, *shard.shape)),
        axes, 0, 0, tiled=True, axis_index_groups=groups,
    )


def product_kernel(a_own, a_oth, v00, v10, v01, v11, out, a_all, v_all):
    px = lax.axis_index("x") % 2
    py = lax.axis_index("ij") % 2
    c = lax.axis_index("c")
    for u, ref in enumerate((a_own, a_oth)):
        for j in range(4):
            start = pl.multiple_of((2 * j + (py + u) % 2) * 256, 256)
            a_all[:, pl.ds(start, 256)] = ref[j]
    for s, t, ref in ((0, 0, v00), (1, 0, v10), (0, 1, v01), (1, 1, v11)):
        offset = ((px + s) % 2) * 128 + ((c + t) % 2) * 64
        for y in range(8):
            start = pl.multiple_of(offset + y * 256, 64)
            v_all[pl.ds(start, 64), :] = ref[y]

    @pl.when(lax.axis_index("kl") == 3)
    def _():
        v_all[pl.ds(1984, 64), :] = jnp.zeros((64, v_all.shape[1]), jnp.bfloat16)

    width = out.shape[2]
    for k in range(4):
        prod = jnp.dot(
            a_all[...], v_all[:, k * width : (k + 1) * width],
            preferred_element_type=jnp.float32,
        )
        out[k] = prod * SCALE


def product(a_own, a_oth, v00, v10, v01, v11):
    n = v00.shape[2]
    return pl.pallas_call(
        product_kernel,
        out_shape=jax.ShapeDtypeStruct((4, 512, n // 4), jnp.float32),
        in_specs=[pl.BlockSpec(memory_space=pltpu.VMEM)] * 6,
        out_specs=pl.BlockSpec(memory_space=pltpu.VMEM),
        scratch_shapes=[
            pltpu.VMEM((512, 2048), jnp.bfloat16),
            pltpu.VMEM((2048, n), jnp.bfloat16),
        ],
        cost_estimate=pl.CostEstimate(
            flops=2 * 512 * 2048 * n, bytes_accessed=4 << 20, transcendentals=0
        ),
    )(a_own, a_oth, v00, v10, v01, v11)


def staged(amplitudes, integrals):
    width = 256 // HALVES
    a_own = to_all(amplitudes, "ij", Y_PARITY, 4)
    a_oth = lax.ppermute(a_own, ("c", "ij"), Y_HOP)
    columns = integrals.reshape(64, 4, HALVES, width)
    owned = []
    for h in range(HALVES):
        part = columns[:, :, h, :].reshape(64, 4 * width)
        v00 = to_all(part, ("zl", "x"), X_PARITY, 8)
        v10 = lax.ppermute(v00, ("x", "c"), X_HOP)
        v01 = lax.ppermute(v00, "c", SWAP)
        v11 = lax.ppermute(v10, "c", SWAP)
        terms = product(a_own, a_oth, v00, v10, v01, v11).astype(jnp.float16)
        got = lax.all_to_all(terms, "kl", 0, 0, tiled=True).astype(jnp.float32)
        owned.append(((got[0] + got[1]) + (got[2] + got[3])) * (1.0 / SCALE))
    owned = jnp.concatenate(owned, axis=1)
    out_ids = lax.axis_index("ij") * 1024 + lax.axis_index("kl") * 256 + jnp.arange(256)
    return jnp.where((out_ids < PAIRS)[None, :], owned, jnp.float32(0.0))


def solution(mesh):
    fine = Mesh(mesh.devices.reshape(2, 8, 2, 4, 8), AXES)
    ab = ("zl", "x", "c")
    return jax.shard_map(
        staged, mesh=fine,
        in_specs=(P(ab, ("kl", "ij")), P(("kl", *ab), "ij")),
        out_specs=P(ab, ("ij", "kl")), check_vma=False,
    )
```

```python
import jax
import jax.numpy as jnp
from jax import lax
from jax.experimental import pallas as pl
from jax.experimental.pallas import tpu as pltpu
from jax.sharding import Mesh
from jax.sharding import PartitionSpec as P


PAIRS = 8128
AXES = ("zl", "x", "c", "kl", "ij")
SCALE = 64.0

X_PARITY = [[zl * 8 + x for zl in range(2) for x in range(p, 8, 2)] for p in range(2)]
Y_HOP = [(c * 8 + y, c * 8 + (y + 1 - 2 * c) % 8) for c in range(2) for y in range(8)]
X_HOP = [(x * 2 + c, (x + 1 - 2 * c) % 8 * 2 + c) for c in range(2) for x in range(8)]
SWAP = [(0, 1), (1, 0)]


def along_y(shard, step):
    return lax.ppermute(shard, "ij", [(y, (y + step) % 8) for y in range(8)])


def product_kernel(*refs):
    a_refs, v_refs, (out, own, a_all, v_all) = refs[:8], refs[8:12], refs[12:]
    x, y, c = (lax.axis_index(name) for name in ("x", "ij", "c"))
    kl = lax.axis_index("kl")
    near = 2 * c - 1
    places = [0, -2, 2, 4]
    places += [near + place for place in places]
    for place, ref in zip(places, a_refs):
        start = pl.multiple_of((y + place + 16) % 8 * 256, 256)
        a_all[:, pl.ds(start, 256)] = ref[...]
    for s, t, ref in ((0, 0, v_refs[0]), (1, 0, v_refs[1]), (0, 1, v_refs[2]), (1, 1, v_refs[3])):
        offset = (x + s) % 2 * 128 + (c + t) % 2 * 64
        for k in range(8):
            start = pl.multiple_of(offset + k * 256, 64)
            v_all[pl.ds(start, 64), :] = ref[k]

    @pl.when(kl == 3)
    def _():
        v_all[pl.ds(1984, 64), :] = jnp.zeros((64, 1024), jnp.bfloat16)

    for k in range(4):
        out[k] = SCALE * jnp.dot(
            a_all[...], v_all[:, k * 256 : (k + 1) * 256],
            preferred_element_type=jnp.float32,
        )
    own[...] = out[kl]


def product(*pieces):
    return pl.pallas_call(
        product_kernel,
        out_shape=(
            jax.ShapeDtypeStruct((4, 512, 256), jnp.float32),
            jax.ShapeDtypeStruct((512, 256), jnp.float32),
        ),
        in_specs=[pl.BlockSpec(memory_space=pltpu.VMEM)] * 12,
        out_specs=[pl.BlockSpec(memory_space=pltpu.VMEM)] * 2,
        scratch_shapes=[
            pltpu.VMEM((512, 2048), jnp.bfloat16),
            pltpu.VMEM((2048, 1024), jnp.bfloat16),
        ],
        compiler_params=pltpu.CompilerParams(vmem_limit_bytes=24 << 20),
        cost_estimate=pl.CostEstimate(
            flops=2 * 512 * 2048 * 1024, bytes_accessed=8 << 20, transcendentals=0
        ),
    )(*pieces)


def untouched_kernel(given, out):
    del given, out


def untouched(block):
    return pl.pallas_call(
        untouched_kernel,
        out_shape=jax.ShapeDtypeStruct(block.shape, block.dtype),
        in_specs=[pl.BlockSpec(memory_space=pl.ANY)],
        out_specs=pl.BlockSpec(memory_space=pl.ANY),
        input_output_aliases={0: 0},
        compiler_params=pltpu.CompilerParams(vmem_limit_bytes=1 << 20),
        cost_estimate=pl.CostEstimate(flops=1000, bytes_accessed=0, transcendentals=0),
    )(block)


def staged(amplitudes, integrals):
    v00 = lax.all_to_all(
        jnp.broadcast_to(integrals[None], (8, 64, 1024)), ("zl", "x"), 0, 0,
        tiled=True, axis_index_groups=X_PARITY,
    )
    blocks = [amplitudes]
    for step in (2, -2, 4):
        blocks.append(along_y(amplitudes, step))
    for i in range(4):
        blocks.append(lax.ppermute(blocks[i], ("c", "ij"), Y_HOP))
        if i == 0:
            blocks[4] = untouched(blocks[4])
    v10 = lax.ppermute(v00, ("x", "c"), X_HOP)
    v01 = lax.ppermute(v00, "c", SWAP)
    v11 = lax.ppermute(v10, "c", SWAP)
    terms, own = product(*blocks, v00, v10, v01, v11)
    terms = terms.astype(jnp.float16)
    kl = lax.axis_index("kl")
    got = lax.all_to_all(terms, "kl", 0, 0, tiled=True)
    total = own
    for k in range(4):
        total = total + jnp.where(kl == k, 0.0, got[k].astype(jnp.float32))
    out_ids = lax.axis_index("ij") * 1024 + kl * 256 + jnp.arange(256)
    return jnp.where((out_ids < PAIRS)[None, :], total * (1.0 / SCALE), jnp.float32(0.0))


def solution(mesh):
    fine = Mesh(mesh.devices.reshape(2, 8, 2, 4, 8), AXES)
    ab = ("zl", "x", "c")
    return jax.shard_map(
        staged, mesh=fine,
        in_specs=(P(ab, ("kl", "ij")), P(("kl", *ab), "ij")),
        out_specs=P(ab, ("ij", "kl")), check_vma=False,
    )
```

```python
import jax
import jax.numpy as jnp
from jax import lax
from jax.experimental import pallas as pl
from jax.experimental.pallas import tpu as pltpu
from jax.sharding import Mesh
from jax.sharding import PartitionSpec as P


PAIRS = 8128
AXES = ("zl", "x", "c", "kl", "ij")
SCALE = 64.0

X_PARITY = [[zl * 8 + x for zl in range(2) for x in range(p, 8, 2)] for p in range(2)]
Y_HOP = [(c * 8 + y, c * 8 + (y + 1 - 2 * c) % 8) for c in range(2) for y in range(8)]
X_HOP = [(x * 2 + c, (x + 1 - 2 * c) % 8 * 2 + c) for c in range(2) for x in range(8)]
SWAP = [(0, 1), (1, 0)]


def along_y(shard, step):
    return lax.ppermute(shard, "ij", [(y, (y + step) % 8) for y in range(8)])


def shifted(term, ahead):
    pairs = [(k, (k + ahead) % 4) for k in range(4)]
    return lax.ppermute(term.astype(jnp.float16), "kl", pairs).astype(jnp.float32)


def first_kernel(*refs):
    a_refs, v_refs, (a_all, v_all) = refs[:8], refs[8:12], refs[12:14]
    x, y, c = (lax.axis_index(name) for name in ("x", "ij", "c"))
    near = 2 * c - 1
    places = [0, -2, 2, 4]
    places += [near + place for place in places]
    for place, ref in zip(places, a_refs):
        start = pl.multiple_of((y + place + 16) % 8 * 256, 256)
        a_all[:, pl.ds(start, 256)] = ref[...]
    for s, t, ref in ((0, 0, v_refs[0]), (1, 0, v_refs[1]), (0, 1, v_refs[2]), (1, 1, v_refs[3])):
        offset = (x + s) % 2 * 128 + (c + t) % 2 * 64
        for k in range(8):
            start = pl.multiple_of(offset + k * 256, 64)
            v_all[pl.ds(start, 64), :] = ref[k]

    @pl.when(lax.axis_index("kl") == 3)
    def _():
        v_all[pl.ds(1984, 64), :] = jnp.zeros((64, 1024), jnp.bfloat16)


    place_product(2, a_all, v_all, refs[14])


def place_product(ahead, a_all, v_all, out):
    start = pl.multiple_of((lax.axis_index("kl") + ahead) % 4 * 256, 256)
    out[...] = SCALE * jnp.dot(
        a_all[...], v_all[:, pl.ds(start, 256)], preferred_element_type=jnp.float32
    )


def later_kernel(a_all, v_all, *outs):
    for ahead, out in zip((1, 3, 0), outs):
        place_product(ahead, a_all, v_all, out)


VMEM = pl.BlockSpec(memory_space=pltpu.VMEM)
TERM = jax.ShapeDtypeStruct((512, 256), jnp.float32)


def first_product(*pieces):
    return pl.pallas_call(
        first_kernel,
        out_shape=(
            jax.ShapeDtypeStruct((512, 2048), jnp.bfloat16),
            jax.ShapeDtypeStruct((2048, 1024), jnp.bfloat16),
            TERM,
        ),
        in_specs=[VMEM] * 12,
        out_specs=[VMEM] * 3,
        compiler_params=pltpu.CompilerParams(vmem_limit_bytes=16 << 20),
        cost_estimate=pl.CostEstimate(
            flops=2 * 512 * 2048 * 256, bytes_accessed=12 << 20, transcendentals=0
        ),
    )(*pieces)


def later_products(a_all, v_all):
    return pl.pallas_call(
        later_kernel,
        out_shape=(TERM,) * 3,
        in_specs=[VMEM] * 2,
        out_specs=[VMEM] * 3,
        compiler_params=pltpu.CompilerParams(vmem_limit_bytes=16 << 20),
        cost_estimate=pl.CostEstimate(
            flops=6 * 512 * 2048 * 256, bytes_accessed=8 << 20, transcendentals=0
        ),
    )(a_all, v_all)


def untouched_kernel(given, out):
    del given, out


def untouched(block):
    return pl.pallas_call(
        untouched_kernel,
        out_shape=jax.ShapeDtypeStruct(block.shape, block.dtype),
        in_specs=[pl.BlockSpec(memory_space=pl.ANY)],
        out_specs=pl.BlockSpec(memory_space=pl.ANY),
        input_output_aliases={0: 0},
        compiler_params=pltpu.CompilerParams(vmem_limit_bytes=1 << 20),
        cost_estimate=pl.CostEstimate(flops=1000, bytes_accessed=0, transcendentals=0),
    )(block)


def staged(amplitudes, integrals):
    v00 = lax.all_to_all(
        jnp.broadcast_to(integrals[None], (8, 64, 1024)), ("zl", "x"), 0, 0,
        tiled=True, axis_index_groups=X_PARITY,
    )
    blocks = [amplitudes]
    for step in (2, -2, 4):
        blocks.append(along_y(amplitudes, step))
    for i in range(4):
        blocks.append(lax.ppermute(blocks[i], ("c", "ij"), Y_HOP))
        if i == 0:
            blocks[4] = untouched(blocks[4])
    v10 = lax.ppermute(v00, ("x", "c"), X_HOP)
    v01 = lax.ppermute(v00, "c", SWAP)
    v11 = lax.ppermute(v10, "c", SWAP)
    a_all, v_all, term = first_product(*blocks, v00, v10, v01, v11)
    total = [shifted(term, 2)]
    term_1, term_3, own = later_products(a_all, v_all)
    total.append(shifted(term_1, 1))
    total.append(shifted(term_3, 3))
    total = own + (total[1] + total[2]) + total[0]
    kl = lax.axis_index("kl")
    out_ids = lax.axis_index("ij") * 1024 + kl * 256 + jnp.arange(256)
    return jnp.where((out_ids < PAIRS)[None, :], total * (1.0 / SCALE), jnp.float32(0.0))


def solution(mesh):
    fine = Mesh(mesh.devices.reshape(2, 8, 2, 4, 8), AXES)
    ab = ("zl", "x", "c")
    return jax.shard_map(
        staged, mesh=fine,
        in_specs=(P(ab, ("kl", "ij")), P(("kl", *ab), "ij")),
        out_specs=P(ab, ("ij", "kl")), check_vma=False,
    )
```

```python
import jax
import jax.numpy as jnp
from jax import lax
from jax.experimental import pallas as pl
from jax.experimental.pallas import tpu as pltpu
from jax.sharding import Mesh
from jax.sharding import PartitionSpec as P


PAIRS = 8128
AXES = ("zl", "x", "c", "kl", "ij")
SCALE = 64.0

X_PARITY = [[zl * 8 + x for zl in range(2) for x in range(p, 8, 2)] for p in range(2)]
X_HOP = [(x * 2 + c, (x + 1 - 2 * c) % 8 * 2 + c) for c in range(2) for x in range(8)]
SWAP = [(0, 1), (1, 0)]


def along_y(shard, hops):
    pairs = [
        (c * 8 + y, c * 8 + (y + hops * (1 - 2 * c)) % 8)
        for c in range(2) for y in range(8)
    ]
    return lax.ppermute(shard, ("c", "ij"), pairs)


def product_kernel(*refs):
    a_refs, v_refs, (out, own, a_all, v_all) = refs[:8], refs[8:12], refs[12:]
    x, y, c = (lax.axis_index(name) for name in ("x", "ij", "c"))
    kl = lax.axis_index("kl")
    for place, ref in zip((0, 2, 4, 6, 1, 3, 5, 7), a_refs):
        start = pl.multiple_of((y + (2 * c - 1) * place + 8) % 8 * 256, 256)
        a_all[:, pl.ds(start, 256)] = ref[...]
    for s, t, ref in ((0, 0, v_refs[0]), (1, 0, v_refs[1]), (0, 1, v_refs[2]), (1, 1, v_refs[3])):
        offset = (x + s) % 2 * 128 + (c + t) % 2 * 64
        for k in range(8):
            start = pl.multiple_of(offset + k * 256, 64)
            v_all[pl.ds(start, 64), :] = ref[k]

    @pl.when(kl == 3)
    def _():
        v_all[PAIRS - 6144 :, :] = jnp.zeros((8192 - PAIRS, 1024), jnp.bfloat16)

    @pl.when(y == 7)
    def _():
        kept = lax.broadcasted_iota(jnp.int32, (2048, 128), 1) < PAIRS - 7168 - 896
        last = v_all[:, 896:].astype(jnp.float32)
        v_all[:, 896:] = jnp.where(kept, last, 0.0).astype(jnp.bfloat16)

    for k in range(4):
        out[k] = SCALE * jnp.dot(
            a_all[...], v_all[:, k * 256 : (k + 1) * 256],
            preferred_element_type=jnp.float32,
        )
    own[...] = out[kl]
    out[kl] = jnp.zeros((512, 256), jnp.float32)


VMEM = pl.BlockSpec(memory_space=pltpu.VMEM)


def product(*pieces):
    return pl.pallas_call(
        product_kernel,
        out_shape=(
            jax.ShapeDtypeStruct((4, 512, 256), jnp.float32),
            jax.ShapeDtypeStruct((512, 256), jnp.float32),
        ),
        in_specs=[VMEM] * 12,
        out_specs=[VMEM] * 2,
        scratch_shapes=[
            pltpu.VMEM((512, 2048), jnp.bfloat16),
            pltpu.VMEM((2048, 1024), jnp.bfloat16),
        ],
        compiler_params=pltpu.CompilerParams(vmem_limit_bytes=24 << 20),
        cost_estimate=pl.CostEstimate(
            flops=2 * 512 * 2048 * 1024, bytes_accessed=8 << 20, transcendentals=0
        ),
    )(*pieces)


def untouched_kernel(given, out):
    del given, out


def untouched(block):
    return pl.pallas_call(
        untouched_kernel,
        out_shape=jax.ShapeDtypeStruct(block.shape, block.dtype),
        in_specs=[pl.BlockSpec(memory_space=pl.ANY)],
        out_specs=pl.BlockSpec(memory_space=pl.ANY),
        input_output_aliases={0: 0},
        compiler_params=pltpu.CompilerParams(vmem_limit_bytes=1 << 20),
        cost_estimate=pl.CostEstimate(flops=1000, bytes_accessed=0, transcendentals=0),
    )(block)


def staged(amplitudes, integrals):
    v00 = lax.all_to_all(
        jnp.broadcast_to(integrals[None], (8, 64, 1024)), ("zl", "x"), 0, 0,
        tiled=True, axis_index_groups=X_PARITY,
    )
    blocks = [amplitudes]
    for i in range(3):
        blocks.append(along_y(blocks[i], 2))
    for i in range(4):
        block = along_y(blocks[i], 1)
        if i == 0:
            block = untouched(block)
        blocks.append(block)
    v10 = lax.ppermute(v00, ("x", "c"), X_HOP)
    v01 = lax.ppermute(v00, "c", SWAP)
    v11 = lax.ppermute(v10, "c", SWAP)
    terms, own = product(*blocks, v00, v10, v01, v11)
    got = lax.all_to_all(terms.astype(jnp.float16), "kl", 0, 0, tiled=True)
    got = got.astype(jnp.float32)
    return ((got[0] + got[1]) + (got[2] + got[3]) + own) * (1.0 / SCALE)


def solution(mesh):
    fine = Mesh(mesh.devices.reshape(2, 8, 2, 4, 8), AXES)
    ab = ("zl", "x", "c")
    return jax.shard_map(
        staged, mesh=fine,
        in_specs=(P(ab, ("kl", "ij")), P(("kl", *ab), "ij")),
        out_specs=P(ab, ("ij", "kl")), check_vma=False,
    )
```

```python
import jax
import jax.numpy as jnp
from jax import lax
from jax.experimental import pallas as pl
from jax.experimental.pallas import tpu as pltpu
from jax.sharding import Mesh
from jax.sharding import PartitionSpec as P


PAIRS = 8128
AXES = ("zl", "x", "c", "kl", "ij")
SCALE = 64.0

X_PARITY = [[zl * 8 + x for zl in range(2) for x in range(p, 8, 2)] for p in range(2)]
X_HOP = [(x * 2 + c, (x + 1 - 2 * c) % 8 * 2 + c) for c in range(2) for x in range(8)]
SWAP = [(0, 1), (1, 0)]


def along_y(shard, hops):
    pairs = [
        (c * 8 + y, c * 8 + (y + hops * (1 - 2 * c)) % 8)
        for c in range(2) for y in range(8)
    ]
    return lax.ppermute(shard, ("c", "ij"), pairs)


def product_kernel(*refs):
    a_refs, v_refs, (out, own, a_all, v_all) = refs[:6], refs[6:10], refs[10:]
    x, y, c = (lax.axis_index(name) for name in ("x", "ij", "c"))
    kl = lax.axis_index("kl")
    a_blocks = [ref[...] for ref in a_refs[:4]]
    a_blocks += [ref[i] for ref in a_refs[4:] for i in range(2)]
    for place, block in zip((0, 2, 4, 6, 1, 3, 5, 7), a_blocks):
        start = pl.multiple_of((y + (2 * c - 1) * place + 8) % 8 * 256, 256)
        a_all[:, pl.ds(start, 256)] = block
    for s, t, ref in ((0, 0, v_refs[0]), (1, 0, v_refs[1]), (0, 1, v_refs[2]), (1, 1, v_refs[3])):
        offset = (x + s) % 2 * 128 + (c + t) % 2 * 64
        for k in range(8):
            start = pl.multiple_of(offset + k * 256, 64)
            v_all[pl.ds(start, 64), :] = ref[k]

    @pl.when(kl == 3)
    def _():
        v_all[PAIRS - 6144 :, :] = jnp.zeros((8192 - PAIRS, 1024), jnp.bfloat16)

    @pl.when(y == 7)
    def _():
        kept = lax.broadcasted_iota(jnp.int32, (2048, 128), 1) < PAIRS - 7168 - 896
        last = v_all[:, 896:].astype(jnp.float32)
        v_all[:, 896:] = jnp.where(kept, last, 0.0).astype(jnp.bfloat16)

    for k in range(4):
        out[k] = SCALE * jnp.dot(
            a_all[...], v_all[:, k * 256 : (k + 1) * 256],
            preferred_element_type=jnp.float32,
        )
    own[...] = out[kl]
    out[kl] = jnp.zeros((512, 256), jnp.float32)


VMEM = pl.BlockSpec(memory_space=pltpu.VMEM)


def product(*pieces):
    return pl.pallas_call(
        product_kernel,
        out_shape=(
            jax.ShapeDtypeStruct((4, 512, 256), jnp.float32),
            jax.ShapeDtypeStruct((512, 256), jnp.float32),
        ),
        in_specs=[VMEM] * 10,
        out_specs=[VMEM] * 2,
        scratch_shapes=[
            pltpu.VMEM((512, 2048), jnp.bfloat16),
            pltpu.VMEM((2048, 1024), jnp.bfloat16),
        ],
        compiler_params=pltpu.CompilerParams(vmem_limit_bytes=24 << 20),
        cost_estimate=pl.CostEstimate(
            flops=2 * 512 * 2048 * 1024, bytes_accessed=8 << 20, transcendentals=0
        ),
    )(*pieces)


def untouched_kernel(given, out):
    del given, out


def untouched(block):
    return pl.pallas_call(
        untouched_kernel,
        out_shape=jax.ShapeDtypeStruct(block.shape, block.dtype),
        in_specs=[pl.BlockSpec(memory_space=pl.ANY)],
        out_specs=pl.BlockSpec(memory_space=pl.ANY),
        input_output_aliases={0: 0},
        compiler_params=pltpu.CompilerParams(vmem_limit_bytes=1 << 20),
        cost_estimate=pl.CostEstimate(flops=1000, bytes_accessed=0, transcendentals=0),
    )(block)


def staged(amplitudes, integrals):
    v00 = lax.all_to_all(
        jnp.broadcast_to(integrals[None], (8, 64, 1024)), ("zl", "x"), 0, 0,
        tiled=True, axis_index_groups=X_PARITY,
    )
    blocks = [amplitudes]
    for i in range(3):
        block = along_y(blocks[i], 2)
        if i == 0:
            block = untouched(block)
        blocks.append(block)
    for i in range(2):
        blocks.append(along_y(jnp.stack(blocks[2 * i : 2 * i + 2]), 1))
    v10 = lax.ppermute(v00, ("x", "c"), X_HOP)
    v01 = lax.ppermute(v00, "c", SWAP)
    v11 = lax.ppermute(v10, "c", SWAP)
    terms, own = product(*blocks, v00, v10, v01, v11)
    got = lax.all_to_all(terms.astype(jnp.float16), "kl", 0, 0, tiled=True)
    got = got.astype(jnp.float32)
    return ((got[0] + got[1]) + (got[2] + got[3]) + own) * (1.0 / SCALE)


def solution(mesh):
    fine = Mesh(mesh.devices.reshape(2, 8, 2, 4, 8), AXES)
    ab = ("zl", "x", "c")
    return jax.shard_map(
        staged, mesh=fine,
        in_specs=(P(ab, ("kl", "ij")), P(("kl", *ab), "ij")),
        out_specs=P(ab, ("ij", "kl")), check_vma=False,
    )
```

```python
import jax
import jax.numpy as jnp
from jax import lax
from jax.experimental import pallas as pl
from jax.experimental.pallas import tpu as pltpu
from jax.sharding import Mesh
from jax.sharding import PartitionSpec as P


PAIRS = 8128
AXES = ("zl", "x", "c", "kl", "ij")
SCALE = 64.0

X_PARITY = [[zl * 8 + x for zl in range(2) for x in range(p, 8, 2)] for p in range(2)]
X_HOP = [(x * 2 + c, (x + 1 - 2 * c) % 8 * 2 + c) for c in range(2) for x in range(8)]
SWAP = [(0, 1), (1, 0)]


def along_y(shard, hops):
    pairs = [
        (c * 8 + y, c * 8 + (y + hops * (1 - 2 * c)) % 8)
        for c in range(2) for y in range(8)
    ]
    return lax.ppermute(shard, ("c", "ij"), pairs)


def shifted(term, ahead):
    pairs = [(k, (k + ahead) % 4) for k in range(4)]
    return lax.ppermute(term.astype(jnp.float16), "kl", pairs).astype(jnp.float32)


def first_kernel(*refs):
    a_refs, v_refs, (a_all, v_all, out, arrived) = refs[:8], refs[8:12], refs[12:]
    x, y, c = (lax.axis_index(name) for name in ("x", "ij", "c"))
    kept = pltpu.make_async_copy(
        a_refs[0], a_all.at[:, pl.ds(pl.multiple_of(y * 256, 256), 256)], arrived
    )
    kept.start()
    for place, ref in zip((2, 4, 6, 1, 3, 5, 7), a_refs[1:]):
        start = pl.multiple_of((y + (2 * c - 1) * place + 8) % 8 * 256, 256)
        a_all[:, pl.ds(start, 256)] = ref[...]
    for s, t, ref in ((0, 0, v_refs[0]), (1, 0, v_refs[1]), (0, 1, v_refs[2]), (1, 1, v_refs[3])):
        offset = (x + s) % 2 * 128 + (c + t) % 2 * 64
        for k in range(8):
            start = pl.multiple_of(offset + k * 256, 64)
            v_all[pl.ds(start, 64), :] = ref[k]

    @pl.when(lax.axis_index("kl") == 3)
    def _():
        v_all[PAIRS - 6144 :, :] = jnp.zeros((8192 - PAIRS, 1024), jnp.bfloat16)

    kept.wait()
    place_product(2, a_all, v_all, out)


def place_product(ahead, a_all, v_all, out):
    start = pl.multiple_of((lax.axis_index("kl") + ahead) % 4 * 256, 256)
    out[...] = SCALE * jnp.dot(
        a_all[...], v_all[:, pl.ds(start, 256)], preferred_element_type=jnp.float32
    )


def later_kernel(a_all, v_all, *outs):
    for ahead, out in zip((1, 3, 0), outs):
        place_product(ahead, a_all, v_all, out)


VMEM = pl.BlockSpec(memory_space=pltpu.VMEM)
TERM = jax.ShapeDtypeStruct((512, 256), jnp.float32)


def first_product(*pieces):
    return pl.pallas_call(
        first_kernel,
        out_shape=(
            jax.ShapeDtypeStruct((512, 2048), jnp.bfloat16),
            jax.ShapeDtypeStruct((2048, 1024), jnp.bfloat16),
            TERM,
        ),
        in_specs=[pl.BlockSpec(memory_space=pl.ANY)] + [VMEM] * 11,
        out_specs=[VMEM] * 3,
        scratch_shapes=[pltpu.SemaphoreType.DMA],
        compiler_params=pltpu.CompilerParams(vmem_limit_bytes=16 << 20),
        cost_estimate=pl.CostEstimate(
            flops=2 * 512 * 2048 * 256, bytes_accessed=12 << 20, transcendentals=0
        ),
    )(*pieces)


def later_products(a_all, v_all):
    return pl.pallas_call(
        later_kernel,
        out_shape=(TERM,) * 3,
        in_specs=[VMEM] * 2,
        out_specs=[VMEM] * 3,
        compiler_params=pltpu.CompilerParams(vmem_limit_bytes=16 << 20),
        cost_estimate=pl.CostEstimate(
            flops=6 * 512 * 2048 * 256, bytes_accessed=8 << 20, transcendentals=0
        ),
    )(a_all, v_all)


def untouched_kernel(given, out):
    del given, out


def untouched(block):
    return pl.pallas_call(
        untouched_kernel,
        out_shape=jax.ShapeDtypeStruct(block.shape, block.dtype),
        in_specs=[pl.BlockSpec(memory_space=pl.ANY)],
        out_specs=pl.BlockSpec(memory_space=pl.ANY),
        input_output_aliases={0: 0},
        compiler_params=pltpu.CompilerParams(vmem_limit_bytes=1 << 20),
        cost_estimate=pl.CostEstimate(flops=1000, bytes_accessed=0, transcendentals=0),
    )(block)


def staged(amplitudes, integrals):
    v00 = lax.all_to_all(
        jnp.broadcast_to(integrals[None], (8, 64, 1024)), ("zl", "x"), 0, 0,
        tiled=True, axis_index_groups=X_PARITY,
    )
    blocks = [amplitudes]
    for i in range(3):
        blocks.append(along_y(blocks[i], 2))
    for i in range(4):
        block = along_y(blocks[i], 1)
        if i == 0:
            block = untouched(block)
        blocks.append(block)
    v10 = lax.ppermute(v00, ("x", "c"), X_HOP)
    v01 = lax.ppermute(v00, "c", SWAP)
    v11 = lax.ppermute(v10, "c", SWAP)
    a_all, v_all, term = first_product(*blocks, v00, v10, v01, v11)
    total = [shifted(term, 2)]
    term_1, term_3, own = later_products(a_all, v_all)
    total.append(shifted(term_1, 1))
    total.append(shifted(term_3, 3))
    total = own + (total[1] + total[2]) + total[0]
    kl = lax.axis_index("kl")
    out_ids = lax.axis_index("ij") * 1024 + kl * 256 + jnp.arange(256)
    return jnp.where((out_ids < PAIRS)[None, :], total * (1.0 / SCALE), jnp.float32(0.0))


def solution(mesh):
    fine = Mesh(mesh.devices.reshape(2, 8, 2, 4, 8), AXES)
    ab = ("zl", "x", "c")
    return jax.shard_map(
        staged, mesh=fine,
        in_specs=(P(ab, ("kl", "ij")), P(("kl", *ab), "ij")),
        out_specs=P(ab, ("ij", "kl")), check_vma=False,
    )
```

```python
import jax
import jax.numpy as jnp
from jax import lax
from jax.experimental import pallas as pl
from jax.experimental.pallas import tpu as pltpu
from jax.sharding import Mesh
from jax.sharding import PartitionSpec as P


PAIRS = 8128
AXES = ("zl", "x", "c", "kl", "ij")
SCALE = 64.0

X_PARITY = [[zl * 8 + x for zl in range(2) for x in range(p, 8, 2)] for p in range(2)]
X_HOP = [(x * 2 + c, (x + 1 - 2 * c) % 8 * 2 + c) for c in range(2) for x in range(8)]
SWAP = [(0, 1), (1, 0)]


def along_y(shard, hops):
    pairs = [
        (c * 8 + y, c * 8 + (y + hops * (1 - 2 * c)) % 8)
        for c in range(2) for y in range(8)
    ]
    return lax.ppermute(shard, ("c", "ij"), pairs)


def shifted(term, ahead):
    pairs = [(k, (k + ahead) % 4) for k in range(4)]
    return lax.ppermute(term.astype(jnp.float16), "kl", pairs).astype(jnp.float32)


def first_kernel(*refs):
    a_refs, v_refs, (a_all, v_all, out) = refs[:8], refs[8:12], refs[12:]
    x, y, c = (lax.axis_index(name) for name in ("x", "ij", "c"))
    for place, ref in zip((0, 2, 4, 6, 1, 3, 5, 7), a_refs):
        start = pl.multiple_of((y + (2 * c - 1) * place + 8) % 8 * 256, 256)
        a_all[:, pl.ds(start, 256)] = ref[...]
    for s, t, ref in ((0, 0, v_refs[0]), (1, 0, v_refs[1]), (0, 1, v_refs[2]), (1, 1, v_refs[3])):
        offset = (x + s) % 2 * 128 + (c + t) % 2 * 64
        for k in range(8):
            start = pl.multiple_of(offset + k * 256, 64)
            v_all[pl.ds(start, 64), :] = ref[k]

    @pl.when(lax.axis_index("kl") == 3)
    def _():
        v_all[PAIRS - 6144 :, :] = jnp.zeros((8192 - PAIRS, 1024), jnp.bfloat16)

    place_product(2, a_all, v_all, out)


def place_product(ahead, a_all, v_all, out):
    start = pl.multiple_of((lax.axis_index("kl") + ahead) % 4 * 256, 256)
    out[...] = SCALE * jnp.dot(
        a_all[...], v_all[:, pl.ds(start, 256)], preferred_element_type=jnp.float32
    )


def later_kernel(a_all, v_all, *outs):
    for ahead, out in zip((1, 3, 0), outs):
        place_product(ahead, a_all, v_all, out)


VMEM = pl.BlockSpec(memory_space=pltpu.VMEM)
TERM = jax.ShapeDtypeStruct((512, 256), jnp.float32)


def first_product(*pieces):
    return pl.pallas_call(
        first_kernel,
        out_shape=(
            jax.ShapeDtypeStruct((512, 2048), jnp.bfloat16),
            jax.ShapeDtypeStruct((2048, 1024), jnp.bfloat16),
            TERM,
        ),
        in_specs=[VMEM] * 12,
        out_specs=[VMEM] * 3,
        compiler_params=pltpu.CompilerParams(vmem_limit_bytes=16 << 20),
        cost_estimate=pl.CostEstimate(
            flops=2 * 512 * 2048 * 256, bytes_accessed=12 << 20, transcendentals=0
        ),
    )(*pieces)


def later_products(a_all, v_all):
    return pl.pallas_call(
        later_kernel,
        out_shape=(TERM,) * 3,
        in_specs=[VMEM] * 2,
        out_specs=[VMEM] * 3,
        compiler_params=pltpu.CompilerParams(vmem_limit_bytes=16 << 20),
        cost_estimate=pl.CostEstimate(
            flops=6 * 512 * 2048 * 256, bytes_accessed=8 << 20, transcendentals=0
        ),
    )(a_all, v_all)


def copies_kernel(given, out, left):
    sends = [pltpu.make_async_copy(given, out.at[i], left.at[i]) for i in range(8)]
    for send in sends:
        send.start()
    for send in sends:
        send.wait()


def copies(shard):
    return pl.pallas_call(
        copies_kernel,
        out_shape=jax.ShapeDtypeStruct((8, *shard.shape), shard.dtype),
        in_specs=[VMEM],
        out_specs=pl.BlockSpec(memory_space=pl.ANY),
        scratch_shapes=[pltpu.SemaphoreType.DMA((8,))],
        compiler_params=pltpu.CompilerParams(vmem_limit_bytes=2 << 20),
        cost_estimate=pl.CostEstimate(
            flops=1000, bytes_accessed=9 << 17, transcendentals=0
        ),
    )(shard)


def kept_kernel(given, own, out, kept):
    del given, out
    kept[...] = own[...]


def kept_beside(block, own):
    shape = jax.ShapeDtypeStruct(block.shape, block.dtype)
    anywhere = pl.BlockSpec(memory_space=pl.ANY)
    return pl.pallas_call(
        kept_kernel,
        out_shape=(shape, shape),
        in_specs=[anywhere, VMEM],
        out_specs=[anywhere, VMEM],
        input_output_aliases={0: 0},
        compiler_params=pltpu.CompilerParams(vmem_limit_bytes=2 << 20),
        cost_estimate=pl.CostEstimate(flops=1000, bytes_accessed=0, transcendentals=0),
    )(block, own)


def staged(amplitudes, integrals):
    v00 = lax.all_to_all(
        copies(integrals), ("zl", "x"), 0, 0,
        tiled=True, axis_index_groups=X_PARITY,
    )
    blocks = [amplitudes]
    for i in range(3):
        blocks.append(along_y(blocks[i], 2))
    for i in range(4):
        block = along_y(blocks[i], 1)
        if i == 0:
            block, kept = kept_beside(block, amplitudes)
        blocks.append(block)
    blocks[0] = kept
    v10 = lax.ppermute(v00, ("x", "c"), X_HOP)
    v01 = lax.ppermute(v00, "c", SWAP)
    v11 = lax.ppermute(v10, "c", SWAP)
    a_all, v_all, term = first_product(*blocks, v00, v10, v01, v11)
    total = [shifted(term, 2)]
    term_1, term_3, own = later_products(a_all, v_all)
    total.append(shifted(term_1, 1))
    total.append(shifted(term_3, 3))
    total = own + (total[1] + total[2]) + total[0]
    kl = lax.axis_index("kl")
    out_ids = lax.axis_index("ij") * 1024 + kl * 256 + jnp.arange(256)
    return jnp.where((out_ids < PAIRS)[None, :], total * (1.0 / SCALE), jnp.float32(0.0))


def solution(mesh):
    fine = Mesh(mesh.devices.reshape(2, 8, 2, 4, 8), AXES)
    ab = ("zl", "x", "c")
    return jax.shard_map(
        staged, mesh=fine,
        in_specs=(P(ab, ("kl", "ij")), P(("kl", *ab), "ij")),
        out_specs=P(ab, ("ij", "kl")), check_vma=False,
    )
```

```python
import jax
import jax.numpy as jnp
from jax import lax
from jax.experimental import pallas as pl
from jax.experimental.pallas import tpu as pltpu
from jax.sharding import Mesh
from jax.sharding import PartitionSpec as P


PAIRS = 8128
AXES = ("zl", "x", "c", "kl", "ij")
SCALE = 64.0

X_PARITY = [[zl * 8 + x for zl in range(2) for x in range(p, 8, 2)] for p in range(2)]
X_HOP = [(x * 2 + c, (x + 1 - 2 * c) % 8 * 2 + c) for c in range(2) for x in range(8)]
SWAP = [(0, 1), (1, 0)]


def along_y(shard, hops):
    pairs = [
        (c * 8 + y, c * 8 + (y + hops * (1 - 2 * c)) % 8)
        for c in range(2) for y in range(8)
    ]
    return lax.ppermute(shard, ("c", "ij"), pairs)


def shifted(term, ahead):
    pairs = [(k, (k + ahead) % 4) for k in range(4)]
    return lax.ppermute(term.astype(jnp.float16), "kl", pairs).astype(jnp.float32)


def first_kernel(*refs):
    a_refs, v_refs, (a_all, v_all, out) = refs[:8], refs[8:12], refs[12:]
    x, y, c = (lax.axis_index(name) for name in ("x", "ij", "c"))
    for place, ref in enumerate(a_refs):
        start = pl.multiple_of((y + (2 * c - 1) * place + 8) % 8 * 256, 256)
        a_all[:, pl.ds(start, 256)] = ref[...]
    for s, t, ref in ((0, 0, v_refs[0]), (1, 0, v_refs[1]), (0, 1, v_refs[2]), (1, 1, v_refs[3])):
        offset = (x + s) % 2 * 128 + (c + t) % 2 * 64
        for k in range(8):
            start = pl.multiple_of(offset + k * 256, 64)
            v_all[pl.ds(start, 64), :] = ref[k]

    @pl.when(lax.axis_index("kl") == 3)
    def _():
        v_all[PAIRS - 6144 :, :] = jnp.zeros((8192 - PAIRS, 1024), jnp.bfloat16)

    place_product(2, a_all, v_all, out)


def place_product(ahead, a_all, v_all, out):
    start = pl.multiple_of((lax.axis_index("kl") + ahead) % 4 * 256, 256)
    out[...] = SCALE * jnp.dot(
        a_all[...], v_all[:, pl.ds(start, 256)], preferred_element_type=jnp.float32
    )


def later_kernel(a_all, v_all, *outs):
    for ahead, out in zip((1, 3, 0), outs):
        place_product(ahead, a_all, v_all, out)


VMEM = pl.BlockSpec(memory_space=pltpu.VMEM)
TERM = jax.ShapeDtypeStruct((512, 256), jnp.float32)


def first_product(*pieces):
    return pl.pallas_call(
        first_kernel,
        out_shape=(
            jax.ShapeDtypeStruct((512, 2048), jnp.bfloat16),
            jax.ShapeDtypeStruct((2048, 1024), jnp.bfloat16),
            TERM,
        ),
        in_specs=[VMEM] * 12,
        out_specs=[VMEM] * 3,
        compiler_params=pltpu.CompilerParams(vmem_limit_bytes=16 << 20),
        cost_estimate=pl.CostEstimate(
            flops=2 * 512 * 2048 * 256, bytes_accessed=12 << 20, transcendentals=0
        ),
    )(*pieces)


def later_products(a_all, v_all):
    return pl.pallas_call(
        later_kernel,
        out_shape=(TERM,) * 3,
        in_specs=[VMEM] * 2,
        out_specs=[VMEM] * 3,
        compiler_params=pltpu.CompilerParams(vmem_limit_bytes=16 << 20),
        cost_estimate=pl.CostEstimate(
            flops=6 * 512 * 2048 * 256, bytes_accessed=8 << 20, transcendentals=0
        ),
    )(a_all, v_all)


def copies_kernel(given, out, left):
    sends = [pltpu.make_async_copy(given, out.at[i], left.at[i]) for i in range(8)]
    for send in sends:
        send.start()
    for send in sends:
        send.wait()


def copies(shard):
    return pl.pallas_call(
        copies_kernel,
        out_shape=jax.ShapeDtypeStruct((8, *shard.shape), shard.dtype),
        in_specs=[VMEM],
        out_specs=pl.BlockSpec(memory_space=pl.ANY),
        scratch_shapes=[pltpu.SemaphoreType.DMA((8,))],
        compiler_params=pltpu.CompilerParams(vmem_limit_bytes=2 << 20),
        cost_estimate=pl.CostEstimate(
            flops=1000, bytes_accessed=9 << 17, transcendentals=0
        ),
    )(shard)


def kept_kernel(given, own, out, kept):
    del given, out
    kept[...] = own[...]


def kept_beside(block, own):
    shape = jax.ShapeDtypeStruct(block.shape, block.dtype)
    anywhere = pl.BlockSpec(memory_space=pl.ANY)
    return pl.pallas_call(
        kept_kernel,
        out_shape=(shape, shape),
        in_specs=[anywhere, VMEM],
        out_specs=[anywhere, VMEM],
        input_output_aliases={0: 0},
        compiler_params=pltpu.CompilerParams(vmem_limit_bytes=2 << 20),
        cost_estimate=pl.CostEstimate(flops=1000, bytes_accessed=0, transcendentals=0),
    )(block, own)


def staged(amplitudes, integrals):
    v00 = lax.all_to_all(
        copies(integrals), ("zl", "x"), 0, 0,
        tiled=True, axis_index_groups=X_PARITY,
    )
    two = along_y(amplitudes, 2)
    one = along_y(amplitudes, 1)
    one, kept = kept_beside(one, amplitudes)
    seven = along_y(amplitudes, -1)
    six = along_y(amplitudes, -2)
    three = along_y(two, 1)
    four = along_y(two, 2)
    five = along_y(six, -1)
    blocks = [kept, one, two, three, four, five, six, seven]
    v10 = lax.ppermute(v00, ("x", "c"), X_HOP)
    v01 = lax.ppermute(v00, "c", SWAP)
    v11 = lax.ppermute(v10, "c", SWAP)
    a_all, v_all, term = first_product(*blocks, v00, v10, v01, v11)
    total = [shifted(term, 2)]
    term_1, term_3, own = later_products(a_all, v_all)
    total.append(shifted(term_1, 1))
    total.append(shifted(term_3, 3))
    total = own + (total[1] + total[2]) + total[0]
    kl = lax.axis_index("kl")
    out_ids = lax.axis_index("ij") * 1024 + kl * 256 + jnp.arange(256)
    return jnp.where((out_ids < PAIRS)[None, :], total * (1.0 / SCALE), jnp.float32(0.0))


def solution(mesh):
    fine = Mesh(mesh.devices.reshape(2, 8, 2, 4, 8), AXES)
    ab = ("zl", "x", "c")
    return jax.shard_map(
        staged, mesh=fine,
        in_specs=(P(ab, ("kl", "ij")), P(("kl", *ab), "ij")),
        out_specs=P(ab, ("ij", "kl")), check_vma=False,
    )
```

```python
import jax
import jax.numpy as jnp
from jax import lax
from jax.experimental import pallas as pl
from jax.experimental.pallas import tpu as pltpu
from jax.sharding import Mesh
from jax.sharding import PartitionSpec as P


PAIRS = 8128
AXES = ("zl", "x", "c", "kl", "ij")
SCALE = 64.0

X_PARITY = [[zl * 8 + x for zl in range(2) for x in range(p, 8, 2)] for p in range(2)]
X_HOP = [(x * 2 + c, (x + 1 - 2 * c) % 8 * 2 + c) for c in range(2) for x in range(8)]
SWAP = [(0, 1), (1, 0)]


def along_y(shard, hops):
    pairs = [
        (c * 8 + y, c * 8 + (y + hops * (1 - 2 * c)) % 8)
        for c in range(2) for y in range(8)
    ]
    return lax.ppermute(shard, ("c", "ij"), pairs)


def shifted(term, ahead):
    pairs = [(k, (k + ahead) % 4) for k in range(4)]
    return lax.ppermute(term.astype(jnp.float16), "kl", pairs).astype(jnp.float32)


def first_kernel(*refs):
    a_refs, v_refs, (a_all, v_all, out_2, out_1) = refs[:8], refs[8:12], refs[12:]
    x, y, c = (lax.axis_index(name) for name in ("x", "ij", "c"))
    for place, ref in enumerate(a_refs):
        start = pl.multiple_of((y + (2 * c - 1) * place + 8) % 8 * 256, 256)
        a_all[:, pl.ds(start, 256)] = ref[...]
    for s, t, ref in ((0, 0, v_refs[0]), (1, 0, v_refs[1]), (0, 1, v_refs[2]), (1, 1, v_refs[3])):
        offset = (x + s) % 2 * 128 + (c + t) % 2 * 64
        for k in range(8):
            start = pl.multiple_of(offset + k * 256, 64)
            v_all[pl.ds(start, 64), :] = ref[k]

    @pl.when(lax.axis_index("kl") == 3)
    def _():
        v_all[PAIRS - 6144 :, :] = jnp.zeros((8192 - PAIRS, 1024), jnp.bfloat16)

    place_product(2, a_all, v_all, out_2)
    place_product(1, a_all, v_all, out_1)


def place_product(ahead, a_all, v_all, out):
    start = pl.multiple_of((lax.axis_index("kl") + ahead) % 4 * 256, 256)
    out[...] = SCALE * jnp.dot(
        a_all[...], v_all[:, pl.ds(start, 256)], preferred_element_type=jnp.float32
    )


def later_kernel(a_all, v_all, *outs):
    for ahead, out in zip((3, 0), outs):
        place_product(ahead, a_all, v_all, out)


VMEM = pl.BlockSpec(memory_space=pltpu.VMEM)
TERM = jax.ShapeDtypeStruct((512, 256), jnp.float32)


def first_product(*pieces):
    return pl.pallas_call(
        first_kernel,
        out_shape=(
            jax.ShapeDtypeStruct((512, 2048), jnp.bfloat16),
            jax.ShapeDtypeStruct((2048, 1024), jnp.bfloat16),
            TERM,
            TERM,
        ),
        in_specs=[VMEM] * 12,
        out_specs=[VMEM] * 4,
        compiler_params=pltpu.CompilerParams(vmem_limit_bytes=16 << 20),
        cost_estimate=pl.CostEstimate(
            flops=4 * 512 * 2048 * 256, bytes_accessed=12 << 20, transcendentals=0
        ),
    )(*pieces)


def later_products(a_all, v_all):
    return pl.pallas_call(
        later_kernel,
        out_shape=(TERM,) * 2,
        in_specs=[VMEM] * 2,
        out_specs=[VMEM] * 2,
        compiler_params=pltpu.CompilerParams(vmem_limit_bytes=16 << 20),
        cost_estimate=pl.CostEstimate(
            flops=4 * 512 * 2048 * 256, bytes_accessed=8 << 20, transcendentals=0
        ),
    )(a_all, v_all)


def copies_kernel(given, out, left):
    sends = [pltpu.make_async_copy(given, out.at[i], left.at[i]) for i in range(8)]
    for send in sends:
        send.start()
    for send in sends:
        send.wait()


def copies(shard):
    return pl.pallas_call(
        copies_kernel,
        out_shape=jax.ShapeDtypeStruct((8, *shard.shape), shard.dtype),
        in_specs=[VMEM],
        out_specs=pl.BlockSpec(memory_space=pl.ANY),
        scratch_shapes=[pltpu.SemaphoreType.DMA((8,))],
        compiler_params=pltpu.CompilerParams(vmem_limit_bytes=2 << 20),
        cost_estimate=pl.CostEstimate(
            flops=1000, bytes_accessed=9 << 17, transcendentals=0
        ),
    )(shard)


def kept_kernel(given, own, out, kept):
    del given, out
    kept[...] = own[...]


def kept_beside(block, own):
    shape = jax.ShapeDtypeStruct(block.shape, block.dtype)
    anywhere = pl.BlockSpec(memory_space=pl.ANY)
    return pl.pallas_call(
        kept_kernel,
        out_shape=(shape, shape),
        in_specs=[anywhere, VMEM],
        out_specs=[anywhere, VMEM],
        input_output_aliases={0: 0},
        compiler_params=pltpu.CompilerParams(vmem_limit_bytes=2 << 20),
        cost_estimate=pl.CostEstimate(flops=1000, bytes_accessed=0, transcendentals=0),
    )(block, own)


def staged(amplitudes, integrals):
    v00 = lax.all_to_all(
        copies(integrals), ("zl", "x"), 0, 0,
        tiled=True, axis_index_groups=X_PARITY,
    )
    two = along_y(amplitudes, 2)
    one = along_y(amplitudes, 1)
    one, kept = kept_beside(one, amplitudes)
    seven = along_y(amplitudes, -1)
    six = along_y(amplitudes, -2)
    three = along_y(two, 1)
    four = along_y(two, 2)
    five = along_y(six, -1)
    blocks = [kept, one, two, three, four, five, six, seven]
    v10 = lax.ppermute(v00, ("x", "c"), X_HOP)
    v01 = lax.ppermute(v00, "c", SWAP)
    v11 = lax.ppermute(v10, "c", SWAP)
    a_all, v_all, term, term_1 = first_product(*blocks, v00, v10, v01, v11)
    total = [shifted(term, 2)]
    total.append(shifted(term_1, 1))
    term_3, own = later_products(a_all, v_all)
    total.append(shifted(term_3, 3))
    total = own + (total[1] + total[2]) + total[0]
    kl = lax.axis_index("kl")
    out_ids = lax.axis_index("ij") * 1024 + kl * 256 + jnp.arange(256)
    return jnp.where((out_ids < PAIRS)[None, :], total * (1.0 / SCALE), jnp.float32(0.0))


def solution(mesh):
    fine = Mesh(mesh.devices.reshape(2, 8, 2, 4, 8), AXES)
    ab = ("zl", "x", "c")
    return jax.shard_map(
        staged, mesh=fine,
        in_specs=(P(ab, ("kl", "ij")), P(("kl", *ab), "ij")),
        out_specs=P(ab, ("ij", "kl")), check_vma=False,
    )
```
